32 devices in a mesh: dp: 8 (over y, x, core), tensor: 4 (over z).
Axes of the slice: x: 2, y: 2, z: 4, core: 2. Of those that a mesh axis runs over, the one named last changes fastest.
Arguments:
- grad_tokens: bfloat16 [1536, 2048], P('dp', 'tensor'), may hold values from -6 to 6
- hidden_input: bfloat16 [2048, 5120], P('dp', 'tensor'), may hold values from -6 to 6
- output_weight: bfloat16 [5120, 2048], P(None, 'tensor'), may hold values from -0.078125 to 0.078125
- image_tokens: int32 [8, 8], replicated, may hold values from 0 to 192, as said below
- moved_images: int32 [8], replicated, may hold values from 0 to 7, as said below
Outputs:
- input_grad: bfloat16 [2048, 5120], P('dp', 'tensor')
- weight_grad: float32 [5120, 2048], P('dp', 'tensor')
- bias_grad: float32 [2048], P('tensor')
The draws below stay inside these ranges and needn't reach their ends.
Inputs may be any that keep to these rules, and one draw needn't show every extreme that they name: `image_tokens`: row s lists the merged tokens of sample s's images in order: 1 to 8 positive entries, then zeros; each row sums to 192. `moved_images`: entry s is less than the number of images of sample s; those trailing images hold at most 64 merged tokens together, exactly 64 for some sample in every draw. They are encoded by owner s + 1 (owner 0 after the last).
All inputs are finite; a program needn't handle non-finite values.
Results may differ from the reference program's by a relative error of at most 0.014.
Values may be sent and summed in bfloat16 or wider, within the bound.
No kernel may reach another device: no remote copies, remote signals or barrier semaphores. Data moves between devices by JAX's collectives and lax.ppermute only.
A program may use at most 64 MiB of HBM per device.

```python
import jax
import jax.numpy as jnp
from jax import lax

HID = 5120
OUT = 2048
IMAGES = 8
TOK_DEV = 192
MOVE_CAP = 64
ROWS = 256
SAMPLES = 8
TOKENS = 1536
BUF = 2048
HPAD = 5120
N_TENSOR = 4


def plan_images(key):
    base = jax.random.fold_in(key, 1234)
    key_count, key_cut, key_high, key_move, key_pick = jax.random.split(base, 5)
    count_images = jax.random.randint(key_count, (SAMPLES,), 1, IMAGES + 1)
    picked = jax.random.randint(key_pick, (), 0, SAMPLES)
    sample_ids = jnp.arange(SAMPLES)
    single = sample_ids == picked
    chosen = sample_ids == (picked + 1) % SAMPLES
    count_images = jnp.where(single, 1, count_images)
    count_images = jnp.where(chosen, IMAGES, count_images)
    free_cuts = jax.vmap(lambda subkey: jax.random.permutation(subkey, TOK_DEV - 1)[:IMAGES - 1] + 1)(jax.random.split(key_cut, SAMPLES))
    high_cuts = jax.random.permutation(key_high, MOVE_CAP - 1)[:IMAGES - 2] + 1 + TOK_DEV - MOVE_CAP
    chosen_cuts = jnp.concatenate([jnp.full((1,), TOK_DEV - MOVE_CAP, high_cuts.dtype), high_cuts])
    slot_ids = jnp.arange(IMAGES - 1)[None, :]
    cuts = jnp.where(chosen[:, None], chosen_cuts[None, :], free_cuts)
    cuts = jnp.where(slot_ids < count_images[:, None] - 1, cuts, TOK_DEV)
    cuts = jnp.sort(cuts, axis=1).astype(jnp.int32)
    bounds = jnp.concatenate([jnp.zeros((SAMPLES, 1), jnp.int32), cuts, jnp.full((SAMPLES, 1), TOK_DEV, jnp.int32)], axis=1)
    sizes = bounds[:, 1:] - bounds[:, :-1]
    trailing = jnp.arange(IMAGES)[None, :]
    start_index = jnp.clip(count_images[:, None] - trailing, 0, IMAGES)
    starts = jnp.take_along_axis(bounds, start_index, axis=1)
    fitting = (TOK_DEV - starts <= MOVE_CAP) & (trailing < count_images[:, None])
    wanted = jax.random.randint(key_move, (SAMPLES,), 0, IMAGES)
    allowed = fitting & (trailing <= wanted[:, None])
    moved = jnp.max(jnp.where(allowed, trailing, 0), axis=1)
    moved = jnp.where(chosen, IMAGES - 1, moved)
    return (sizes.astype(jnp.int32), moved.astype(jnp.int32))


def draw_image_tokens(key, part):
    return plan_images(key)[0]


def draw_moved_images(key, part):
    return plan_images(key)[1]


def raised(drawn, own_key, source, target, shards_of, factor):
    owner, partner = [(jnp.arange(drawn.shape[axis_at]) // (drawn.shape[axis_at] // shards_of)).reshape([-1 if axis == axis_at else 1 for axis in range(drawn.ndim)]) for axis_at in (source, target)]
    chosen = jax.random.permutation(own_key, shards_of)[partner]
    strong = (owner == chosen) | (owner == (partner + shards_of // 2) % shards_of)
    return jnp.where(strong, factor * drawn, drawn)


def block_scale(rng, extent, cuts, least, high):
    level, own = 1.0, jax.random.fold_in(rng, 6)
    for dim, blocks in cuts:
        heights = jnp.exp(jax.random.uniform(jax.random.fold_in(own, dim), (blocks,), jnp.float32, least / len(cuts), high / len(cuts)))
        level = level * jnp.repeat(heights, extent[dim] // blocks).reshape([-1 if axis == dim else 1 for axis in range(len(extent))])
    return level


def bell_draw(rng, shape, spread, bound, shards=(), kind=jnp.bfloat16):
    result = spread * jax.random.normal(rng, shape, jnp.float32)
    if shards:
        result = result * block_scale(rng, shape, shards, -0.22, 0.18)
    return jnp.clip(result, -bound, bound).astype(kind)


def gaussian_with(own_key, dims, scale, limit, pieces, heavy, held_as=jnp.bfloat16):
    entries = scale * jax.random.normal(own_key, dims, jnp.float32)
    if pieces:
        entries = entries * block_scale(own_key, dims, pieces, -0.22, 0.18)
    return jnp.clip(raised(entries, jax.random.fold_in(own_key, 3), *heavy), -limit, limit).astype(held_as)


def setup_inputs(seed: int = 0) -> dict:
    keys = jax.random.split(jax.random.key(seed), 6)
    grad_tokens = bell_draw(keys[0], (TOKENS, OUT), 1.0, 6.0, ((0, 8), (1, 4)))
    hidden_input = gaussian_with(keys[1], (BUF, HID), 1.0, 6.0, ((0, 8), (1, 4)), (0, 1, 8, 2.0))
    output_weight = bell_draw(keys[2], (HID, OUT), HID ** -0.5, 0.078125, ((1, 4),))
    image_tokens = draw_image_tokens(jax.random.fold_in(keys[5], 71), 0)
    moved_images = draw_moved_images(jax.random.fold_in(keys[5], 71), 0)
    return {"grad_tokens": grad_tokens, "hidden_input": hidden_input, "output_weight": output_weight, "image_tokens": image_tokens, "moved_images": moved_images}


root_half = 0.7071067811865476
inv_root_tau = 0.3989422804014327


def gelu_parts(values):
    normal_cdf = 0.5 * (1.0 + jax.scipy.special.erf(values * root_half))
    density = jnp.exp(-0.5 * values * values) * inv_root_tau
    return values * normal_cdf, normal_cdf + values * density


def kept_lengths(image_tokens, moved_images):
    present = jnp.sum((image_tokens > 0).astype(jnp.int32), axis=1)
    slot_ids = jnp.arange(image_tokens.shape[1], dtype=jnp.int32)
    kept_mask = slot_ids[None, :] < (present - moved_images)[:, None]
    return jnp.sum(jnp.where(kept_mask, image_tokens, 0), axis=1).astype(jnp.int32)


def reference(grad_tokens, hidden_input, output_weight, image_tokens, moved_images):
    keep_len = kept_lengths(image_tokens, moved_images)
    grad_blocks = grad_tokens.reshape(SAMPLES, TOK_DEV, OUT)
    positions = jnp.arange(TOK_DEV, dtype=jnp.int32)
    zero_value = jnp.zeros((), jnp.bfloat16)
    kept_rows = jnp.where(positions[None, :, None] < keep_len[:, None, None], grad_blocks, zero_value)
    moving = jnp.where(positions[None, TOK_DEV - MOVE_CAP:, None] >= keep_len[:, None, None],
                       grad_blocks[:, TOK_DEV - MOVE_CAP:], zero_value)
    buffers = jnp.concatenate([kept_rows, jnp.roll(moving, 1, axis=0)], axis=1)
    bias_grad = jnp.sum(grad_tokens.astype(jnp.float32), axis=0)
    inputs = hidden_input.reshape(SAMPLES, ROWS, HID)
    column_width = OUT // N_TENSOR

    def one_owner(running, owner_data):
        grad_rows, input_rows = owner_data
        grad_hidden = jnp.zeros((ROWS, HID), jnp.float32)
        for tensor_block in range(N_TENSOR):
            low = tensor_block * column_width
            partial_value = lax.dot_general(grad_rows[:, low:low + column_width], output_weight[:, low:low + column_width],
                                      (((1,), (1,)), ((), ())), preferred_element_type=jnp.float32)
            rounded = lax.optimization_barrier(partial_value.astype(jnp.bfloat16))
            grad_hidden = grad_hidden + rounded.astype(jnp.float32)
        activation, slopes = gelu_parts(input_rows.astype(jnp.float32))
        activation = activation.astype(jnp.bfloat16)
        input_grad = (grad_hidden * slopes).astype(jnp.bfloat16)
        running = running + lax.dot_general(activation, grad_rows, (((0,), (0,)), ((), ())),
                                            preferred_element_type=jnp.float32)
        return running, input_grad

    weight_sum, input_grads = lax.scan(one_owner, jnp.zeros((HID, OUT), jnp.float32), (buffers, inputs))
    weight_grad = jnp.concatenate([weight_sum, jnp.zeros((HPAD - HID, OUT), jnp.float32)], axis=0)
    return input_grads.reshape(BUF, HID), weight_grad, bias_grad
```

```python
import jax
import jax.numpy as jnp
from jax import lax
from jax.sharding import PartitionSpec as P

root_half = 0.7071067811865476
inv_root_tau = 0.3989422804014327


def from_behind(value, axis, steps):
    count = lax.axis_size(axis)
    pairs = [(source, (source + steps) % count) for source in range(count)]
    return lax.ppermute(value, axis, pairs)


def gelu_parts(values):
    normal_cdf = 0.5 * (1.0 + jax.scipy.special.erf(values * root_half))
    density = jnp.exp(-0.5 * values * values) * inv_root_tau
    return (values * normal_cdf, normal_cdf + values * density)


def kept_lengths(image_tokens, moved_images):
    present = jnp.sum((image_tokens > 0).astype(jnp.int32), axis=1)
    slot_ids = jnp.arange(image_tokens.shape[1], dtype=jnp.int32)
    kept_mask = slot_ids[None, :] < (present - moved_images)[:, None]
    return jnp.sum(jnp.where(kept_mask, image_tokens, 0), axis=1)


def native_form(grad_tokens, hidden_input, output_weight, image_tokens, moved_images):
    dp_count = lax.axis_size("dp")
    dp_index = lax.axis_index("dp")
    tok_rows = grad_tokens.shape[0]
    buffer_rows = hidden_input.shape[0]
    tail_count = buffer_rows - tok_rows
    keep_len = kept_lengths(image_tokens, moved_images)
    own_keep = jnp.sum(jnp.where(jnp.arange(dp_count, dtype=jnp.int32) == dp_index, keep_len, 0))
    positions = jnp.arange(tok_rows, dtype=jnp.int32)[:, None]
    zero_value = jnp.zeros((), jnp.bfloat16)
    kept_rows = jnp.where(positions < own_keep, grad_tokens, zero_value)
    moving = jnp.where(
        positions[tok_rows - tail_count :] >= own_keep,
        grad_tokens[tok_rows - tail_count :],
        zero_value,
    )
    arrived = from_behind(moving, "dp", 1)
    grad_rows = jnp.concatenate([kept_rows, arrived], axis=0)
    bias_grad = lax.psum(jnp.sum(grad_tokens.astype(jnp.float32), axis=0), "dp")
    activation, slopes = gelu_parts(hidden_input.astype(jnp.float32))
    partials = lax.dot_general(
        grad_rows, output_weight, (((1,), (1,)), ((), ())), preferred_element_type=jnp.float32
    )
    grad_hidden = lax.psum_scatter(
        partials.astype(jnp.bfloat16), "tensor", scatter_dimension=1, tiled=True
    ).astype(jnp.float32)
    input_grad = (grad_hidden * slopes).astype(jnp.bfloat16)
    gathered_input = lax.all_gather(hidden_input, "tensor", axis=1, tiled=True)
    full_act = gelu_parts(gathered_input.astype(jnp.float32))[0].astype(jnp.bfloat16)
    hidden_width = full_act.shape[1]
    rows_each = (hidden_width + 8 * dp_count - 1) // (8 * dp_count) * 8
    padded = jnp.pad(full_act, ((0, 0), (0, rows_each * dp_count - hidden_width)))
    weight_grad = lax.psum_scatter(
        lax.dot_general(
            padded, grad_rows, (((0,), (0,)), ((), ())), preferred_element_type=jnp.float32
        ),
        "dp",
        scatter_dimension=0,
        tiled=True,
    )
    return (input_grad, weight_grad, bias_grad)


def shifted(value, steps):
    return from_behind(value, "tensor", steps)


def swapped(value, mask):
    count = lax.axis_size("dp")
    return lax.ppermute(value, "dp", [(source, source ^ mask) for source in range(count)])


def gathered_blocks(own, count):
    blocks = {0: own}
    for mask in range(2, count, 2):
        blocks[mask] = swapped(own, mask)
    for mask in range(0, count, 2):
        blocks[mask + 1] = swapped(blocks[mask], 1)
    return [blocks[mask] for mask in range(count)]


def exchanged_form(grad_tokens, hidden_input, output_weight, image_tokens, moved_images):
    dp_count = lax.axis_size("dp")
    dp_index = lax.axis_index("dp")
    t_count = lax.axis_size("tensor")
    t_index = lax.axis_index("tensor")
    tok_rows, out_width = grad_tokens.shape
    buffer_rows, hid_width = hidden_input.shape
    tail_count = buffer_rows - tok_rows
    head = tok_rows - tail_count
    hidden = output_weight.shape[0]
    rows_each = hidden // dp_count
    part_rows = hid_width // dp_count
    per_block = dp_count // t_count
    zero_value = jnp.zeros((), jnp.bfloat16)

    w_parts = []
    for steps in range(1, t_count):
        first = ((t_index + steps) % t_count) * hid_width + dp_index * part_rows
        w_parts.append(shifted(lax.dynamic_slice(output_weight, (first, 0), (part_rows, out_width)), steps))

    keep_len = kept_lengths(image_tokens, moved_images)
    own_keep = jnp.sum(jnp.where(jnp.arange(dp_count, dtype=jnp.int32) == dp_index, keep_len, 0))
    tail_positions = jnp.arange(head, tok_rows, dtype=jnp.int32)[:, None]
    stays = tail_positions < own_keep

    act = gelu_parts(hidden_input.astype(jnp.float32))[0].astype(jnp.bfloat16)
    next_tail = from_behind(act[tok_rows:], "dp", dp_count - 1)
    act_parts = [act[:head], jnp.where(stays, act[head:tok_rows], next_tail)]

    moving = jnp.where(stays, zero_value, grad_tokens[head:])
    arrived = from_behind(moving, "dp", 1)
    grad_rows = jnp.concatenate(
        [grad_tokens[:head], jnp.where(stays, grad_tokens[head:], zero_value), arrived], axis=0
    )

    tokens = gathered_blocks(grad_tokens, dp_count)
    bias_grad = sum(jnp.sum(block.astype(jnp.float32), axis=0) for block in tokens)

    w_blocks = gathered_blocks(jnp.concatenate(w_parts, axis=1), dp_count)

    weight_grad = None
    low = 0
    for part in act_parts:
        rows = part.shape[0]
        ring = jnp.stack([part] + [shifted(part, steps) for steps in range(1, t_count)])
        pieces = []
        for mask in range(dp_count):
            target = dp_index ^ mask
            steps = (t_index - target // per_block) % t_count
            piece = lax.dynamic_slice(
                ring, (steps, 0, (target % per_block) * rows_each), (1, rows, rows_each)
            )[0]
            pieces.append(swapped(piece, mask) if mask else piece)
        grads = [block[low : low + rows] for block in tokens]
        added = lax.dot_general(
            jnp.concatenate(pieces, axis=0),
            jnp.concatenate(grads, axis=0),
            (((0,), (0,)), ((), ())),
            preferred_element_type=jnp.float32,
        )
        weight_grad = added if weight_grad is None else weight_grad + added
        low += rows

    w_other = jnp.zeros((hid_width, (t_count - 1) * out_width), jnp.bfloat16)
    for mask in range(dp_count):
        w_other = lax.dynamic_update_slice(w_other, w_blocks[mask], ((dp_index ^ mask) * part_rows, 0))
    w_own = lax.dynamic_slice(output_weight, (t_index * hid_width, 0), (hid_width, out_width))
    g_other = jnp.concatenate([shifted(grad_rows, steps) for steps in range(1, t_count)], axis=1)
    contract = (((1,), (1,)), ((), ()))
    grad_hidden = lax.dot_general(
        grad_rows, w_own, contract, preferred_element_type=jnp.float32
    ) + lax.dot_general(g_other, w_other, contract, preferred_element_type=jnp.float32)
    slopes = gelu_parts(hidden_input.astype(jnp.float32))[1]
    input_grad = (grad_hidden * slopes).astype(jnp.bfloat16)
    return (input_grad, weight_grad, bias_grad)


def per_device(grad_tokens, hidden_input, output_weight, image_tokens, moved_images):
    dp_count = lax.axis_size("dp")
    t_count = lax.axis_size("tensor")
    hid_width = hidden_input.shape[1]
    fits = (
        dp_count > 1
        and dp_count & (dp_count - 1) == 0
        and t_count > 1
        and dp_count % t_count == 0
        and hid_width % (16 * dp_count) == 0
        and output_weight.shape[0] % (128 * dp_count) == 0
    )
    form = exchanged_form if fits else native_form
    return form(grad_tokens, hidden_input, output_weight, image_tokens, moved_images)


def solution(mesh):
    return jax.shard_map(
        per_device,
        mesh=mesh,
        in_specs=(P("dp", "tensor"), P("dp", "tensor"), P(None, "tensor"), P(), P()),
        out_specs=(P("dp", "tensor"), P("dp", "tensor"), P("tensor")),
        check_vma=False,
    )
```

```python
import jax
import jax.numpy as jnp
from jax import lax
from jax.sharding import PartitionSpec as P

root_half = 0.7071067811865476
inv_root_tau = 0.3989422804014327


def from_behind(value, axis, steps):
    count = lax.axis_size(axis)
    pairs = [(source, (source + steps) % count) for source in range(count)]
    return lax.ppermute(value, axis, pairs)


def gelu_parts(values):
    normal_cdf = 0.5 * (1.0 + jax.scipy.special.erf(values * root_half))
    density = jnp.exp(-0.5 * values * values) * inv_root_tau
    return (values * normal_cdf, normal_cdf + values * density)


def kept_lengths(image_tokens, moved_images):
    present = jnp.sum((image_tokens > 0).astype(jnp.int32), axis=1)
    slot_ids = jnp.arange(image_tokens.shape[1], dtype=jnp.int32)
    kept_mask = slot_ids[None, :] < (present - moved_images)[:, None]
    return jnp.sum(jnp.where(kept_mask, image_tokens, 0), axis=1)


def native_form(grad_tokens, hidden_input, output_weight, image_tokens, moved_images):
    dp_count = lax.axis_size("dp")
    dp_index = lax.axis_index("dp")
    tok_rows = grad_tokens.shape[0]
    buffer_rows = hidden_input.shape[0]
    tail_count = buffer_rows - tok_rows
    keep_len = kept_lengths(image_tokens, moved_images)
    own_keep = jnp.sum(jnp.where(jnp.arange(dp_count, dtype=jnp.int32) == dp_index, keep_len, 0))
    positions = jnp.arange(tok_rows, dtype=jnp.int32)[:, None]
    zero_value = jnp.zeros((), jnp.bfloat16)
    kept_rows = jnp.where(positions < own_keep, grad_tokens, zero_value)
    moving = jnp.where(
        positions[tok_rows - tail_count :] >= own_keep,
        grad_tokens[tok_rows - tail_count :],
        zero_value,
    )
    arrived = from_behind(moving, "dp", 1)
    grad_rows = jnp.concatenate([kept_rows, arrived], axis=0)
    bias_grad = lax.psum(jnp.sum(grad_tokens.astype(jnp.float32), axis=0), "dp")
    _, slopes = gelu_parts(hidden_input.astype(jnp.float32))
    partials = lax.dot_general(
        grad_rows, output_weight, (((1,), (1,)), ((), ())), preferred_element_type=jnp.float32
    )
    grad_hidden = lax.psum_scatter(
        partials.astype(jnp.bfloat16), "tensor", scatter_dimension=1, tiled=True
    ).astype(jnp.float32)
    input_grad = (grad_hidden * slopes).astype(jnp.bfloat16)
    gathered_input = lax.all_gather(hidden_input, "tensor", axis=1, tiled=True)
    full_act = gelu_parts(gathered_input.astype(jnp.float32))[0].astype(jnp.bfloat16)
    hidden_width = full_act.shape[1]
    rows_each = (hidden_width + 8 * dp_count - 1) // (8 * dp_count) * 8
    padded = jnp.pad(full_act, ((0, 0), (0, rows_each * dp_count - hidden_width)))
    weight_grad = lax.psum_scatter(
        lax.dot_general(
            padded, grad_rows, (((0,), (0,)), ((), ())), preferred_element_type=jnp.float32
        ),
        "dp",
        scatter_dimension=0,
        tiled=True,
    )
    return (input_grad, weight_grad, bias_grad)


def shifted(value, steps):
    return from_behind(value, "tensor", steps)


def swapped(value, mask):
    count = lax.axis_size("dp")
    return lax.ppermute(value, "dp", [(source, source ^ mask) for source in range(count)])


def gathered_blocks(own, count):
    blocks = {0: own}
    for mask in range(2, count, 2):
        blocks[mask] = swapped(own, mask)
    for mask in range(0, count, 2):
        blocks[mask + 1] = swapped(blocks[mask], 1)
    return [blocks[mask] for mask in range(count)]


def exchanged_form(grad_tokens, hidden_input, output_weight, image_tokens, moved_images):
    dp_count = lax.axis_size("dp")
    dp_index = lax.axis_index("dp")
    t_count = lax.axis_size("tensor")
    t_index = lax.axis_index("tensor")
    tok_rows, out_width = grad_tokens.shape
    buffer_rows, hid_width = hidden_input.shape
    tail_count = buffer_rows - tok_rows
    head = tok_rows - tail_count
    hidden = output_weight.shape[0]
    rows_each = hidden // dp_count
    part_rows = hid_width // dp_count
    per_block = dp_count // t_count
    zero_value = jnp.zeros((), jnp.bfloat16)

    w_parts = []
    for steps in range(1, t_count):
        first = ((t_index + steps) % t_count) * hid_width + dp_index * part_rows
        w_parts.append(shifted(lax.dynamic_slice(output_weight, (first, 0), (part_rows, out_width)), steps))

    keep_len = kept_lengths(image_tokens, moved_images)
    own_keep = jnp.sum(jnp.where(jnp.arange(dp_count, dtype=jnp.int32) == dp_index, keep_len, 0))
    tail_positions = jnp.arange(head, tok_rows, dtype=jnp.int32)[:, None]
    stays = tail_positions < own_keep

    act = gelu_parts(hidden_input.astype(jnp.float32))[0].astype(jnp.bfloat16)
    next_tail = from_behind(act[tok_rows:], "dp", dp_count - 1)
    act_parts = [act[:head], jnp.where(stays, act[head:tok_rows], next_tail)]

    moving = jnp.where(stays, zero_value, grad_tokens[head:])
    arrived = from_behind(moving, "dp", 1)
    grad_rows = jnp.concatenate(
        [grad_tokens[:head], jnp.where(stays, grad_tokens[head:], zero_value), arrived], axis=0
    )

    tokens = gathered_blocks(grad_tokens, dp_count)
    bias_grad = sum(jnp.sum(block.astype(jnp.float32), axis=0) for block in tokens)

    w_blocks = gathered_blocks(jnp.concatenate(w_parts, axis=1), dp_count)

    weight_grad = None
    low = 0
    for name, part in zip(("head", "tail"), act_parts):
        rows = part.shape[0]
        hops = [part] + [shifted(part, steps) for steps in range(1, t_count) if steps != 2 or name == "tail"]
        if t_count > 2 and name == "head":
            hops.insert(2, shifted(hops[1], 1))
        ring = jnp.stack(hops)
        pieces = []
        for mask in range(dp_count):
            target = dp_index ^ mask
            steps = (t_index - target // per_block) % t_count
            piece = lax.dynamic_slice(
                ring, (steps, 0, (target % per_block) * rows_each), (1, rows, rows_each)
            )[0]
            pieces.append(swapped(piece, mask) if mask else piece)
        grads = [block[low : low + rows] for block in tokens]
        added = lax.dot_general(
            jnp.concatenate(pieces, axis=0),
            jnp.concatenate(grads, axis=0),
            (((0,), (0,)), ((), ())),
            preferred_element_type=jnp.float32,
        )
        weight_grad = added if weight_grad is None else weight_grad + added
        low += rows

    w_other = jnp.zeros((hid_width, (t_count - 1) * out_width), jnp.bfloat16)
    for mask in range(dp_count):
        w_other = lax.dynamic_update_slice(w_other, w_blocks[mask], ((dp_index ^ mask) * part_rows, 0))
    w_own = lax.dynamic_slice(output_weight, (t_index * hid_width, 0), (hid_width, out_width))
    g_other = jnp.concatenate([shifted(grad_rows, steps) for steps in range(1, t_count)], axis=1)
    contract = (((1,), (1,)), ((), ()))
    grad_hidden = lax.dot_general(
        grad_rows, w_own, contract, preferred_element_type=jnp.float32
    ) + lax.dot_general(g_other, w_other, contract, preferred_element_type=jnp.float32)
    slopes = gelu_parts(hidden_input.astype(jnp.float32))[1]
    input_grad = (grad_hidden * slopes).astype(jnp.bfloat16)
    return (input_grad, weight_grad, bias_grad)


def per_device(grad_tokens, hidden_input, output_weight, image_tokens, moved_images):
    dp_count = lax.axis_size("dp")
    t_count = lax.axis_size("tensor")
    hid_width = hidden_input.shape[1]
    fits = (
        dp_count > 1
        and dp_count & (dp_count - 1) == 0
        and t_count > 1
        and dp_count % t_count == 0
        and hid_width % (16 * dp_count) == 0
        and output_weight.shape[0] % (128 * dp_count) == 0
    )
    if not fits:
        return native_form(grad_tokens, hidden_input, output_weight, image_tokens, moved_images)
    return exchanged_form(grad_tokens, hidden_input, output_weight, image_tokens, moved_images)


def solution(mesh):
    return jax.shard_map(
        per_device,
        mesh=mesh,
        in_specs=(P("dp", "tensor"), P("dp", "tensor"), P(None, "tensor"), P(), P()),
        out_specs=(P("dp", "tensor"), P("dp", "tensor"), P("tensor")),
        check_vma=False,
    )
```
